32 devices in a mesh: dp: 4 (over z), tensor: 8 (over y, x, core).
Axes of the slice: x: 2, y: 2, z: 4, core: 2. Of those that a mesh axis runs over, the one named last changes fastest.
Arguments:
- embed_rows: bfloat16 [98304, 512], P('tensor', 'dp'), may hold values from -6 to 6
- head_rows: bfloat16 [98304, 512], P('tensor', 'dp'), may hold values from -6 to 6
- row_offsets: int32 [2, 9], replicated, may hold values from -2047 to 67583, as said below
- slot_table: int32 [1024], replicated, may hold values from 0 to 1023, as said below
- probe: bfloat16 [512, 1024], replicated, may hold values from -0.25 to 0.25
Outputs:
- stored: bfloat16 [1024, 128, 512], P(('dp', 'tensor'))
- sketch: float32 [1024, 128, 1024], P(('dp', 'tensor'))
The draws below stay inside these ranges and needn't reach their ends.
Inputs may be any that keep to these rules, and one draw needn't show every extreme that they name: row_offsets[m, 8] is row_offsets[m, 0] + 65536; every entry row_offsets[m, t] with t < 8 lies strictly within 2048 rows of t * 8192, and the distance 8192 // 4 - 1 is reached above and below among ranks 1 onward in every row of every draw; row_offsets[m, 0] is never 0, above 0 for one matrix and below 0 for the other. `slot_table`: A permutation of the 1024 block numbers. Devices along dp+tensor write 32 consecutive slots each; among one device's slots exactly 4 blocks come from each aligned range of 8192 vocabulary rows (rows t * 8192 onward of either matrix, both matrices together).
All inputs are finite; a program needn't handle non-finite values.
Results may differ from the reference program's by a relative error of at most 0.001.
Values may be sent and summed in bfloat16 or wider, within the bound.
A program may use at most 64 MiB of HBM per device.

```python
import jax
import jax.numpy as jnp
from jax import lax

R = 8192
PW = 1024
BLOCK = 128
CAP = 12288
C = 512
NBLK = 512
N_TENSOR = 8
DEVICES = 32


def draw_row_offsets(key, part):
    first, second, third, fourth, fifth = jax.random.split(key, 5)
    reach = R // 4 - 1
    inner = N_TENSOR - 1
    shifts = jax.random.randint(first, (2, inner), -reach, reach + 1)
    upper = jax.random.randint(second, (2,), 0, inner)
    lower = (upper + 1 + jax.random.randint(third, (2,), 0, inner - 1)) % inner
    column = jnp.arange(inner)[None, :]
    shifts = jnp.where(column == upper[:, None], reach, shifts)
    shifts = jnp.where(column == lower[:, None], -reach, shifts)
    interior = jnp.arange(1, N_TENSOR)[None, :] * R + shifts
    size = jax.random.randint(fourth, (2,), 1, reach + 1)
    flip = jax.random.randint(fifth, (), 0, 2)
    signs = jnp.where(jnp.arange(2) == flip, 1, -1)
    starts = (signs * size).astype(jnp.int32)[:, None]
    ends = starts + R * N_TENSOR
    return jnp.concatenate([starts, interior.astype(jnp.int32), ends], axis=1).astype(jnp.int32)


def draw_slot_table(key, part):
    first, second = jax.random.split(key)
    per_rank = R // BLOCK
    total_blocks = per_rank * N_TENSOR
    slot_count = 2 * total_blocks // DEVICES
    shuffled = jax.random.permutation(first, DEVICES).astype(jnp.int32)
    source = (shuffled[:, None] + jnp.arange(slot_count, dtype=jnp.int32)[None, :]) % N_TENSOR
    flat_source = source.reshape(-1)
    slot_total = DEVICES * slot_count
    noise = jax.random.permutation(second, slot_total).astype(jnp.int32)
    ordering = jnp.argsort(flat_source * slot_total + noise)
    within = jnp.arange(slot_total, dtype=jnp.int32) % (2 * per_rank)
    local_block = jnp.zeros((slot_total,), jnp.int32).at[ordering].set(within)
    result = local_block // per_rank * total_blocks + flat_source * per_rank + local_block % per_rank
    return result.astype(jnp.int32)


def steps_of(own_key, extent, pieces, least, high):
    level = 1.0
    for position, parts in pieces:
        draws = jax.random.uniform(jax.random.fold_in(jax.random.fold_in(own_key, 6), position), (parts,), jnp.float32, least / len(pieces), high / len(pieces))
        level = level * jnp.repeat(jnp.exp(draws), extent[position] // parts).reshape((-1,) + (1,) * (len(extent) - 1 - position))
    return level


def normal_values(own_key, extent, scale, bound, cuts=(), kind=jnp.bfloat16):
    gain = steps_of(own_key, extent, cuts, -0.22, 0.18) if cuts else 1.0
    array = jax.random.normal(own_key, extent, jnp.float32) * scale * gain
    return jnp.minimum(jnp.maximum(array, -bound), bound).astype(kind)


def setup_inputs(seed: int = 0) -> dict:
    seeds = jax.random.split(jax.random.key(seed), 6)
    embed_rows = normal_values(seeds[0], (N_TENSOR * CAP, C), 1.0, 6.0, ((0, 8), (1, 4)))
    head_rows = normal_values(seeds[1], (N_TENSOR * CAP, C), 1.0, 6.0, ((0, 8), (1, 4)))
    row_offsets = draw_row_offsets(jax.random.fold_in(seeds[5], 71), 0)
    slot_table = draw_slot_table(jax.random.fold_in(seeds[5], 71), 0)
    probe = normal_values(seeds[4], (C, PW), C ** -0.5, 0.25)
    return dict(embed_rows=embed_rows, head_rows=head_rows, row_offsets=row_offsets, slot_table=slot_table, probe=probe)


def assemble(buffer, offsets):
    vocab_rows = jnp.arange(R * N_TENSOR, dtype=jnp.int32)
    unwrapped = jnp.where(vocab_rows < offsets[0], vocab_rows + R * N_TENSOR,
                          jnp.where(vocab_rows >= offsets[N_TENSOR], vocab_rows - R * N_TENSOR, vocab_rows)).astype(jnp.int32)
    owner = jnp.sum((offsets[1:N_TENSOR][None, :] <= unwrapped[:, None]).astype(jnp.int32), axis=1).astype(jnp.int32)
    source_row = (owner * CAP + unwrapped - offsets[owner]).astype(jnp.int32)
    return buffer[source_row]


def reference(embed_rows, head_rows, row_offsets, slot_table, probe):
    whole = jnp.concatenate([assemble(embed_rows, row_offsets[0]), assemble(head_rows, row_offsets[1])], axis=0)
    blocks = whole.reshape(2 * NBLK, BLOCK, C)
    stored = blocks[slot_table]
    sketch = jnp.dot(stored.reshape(-1, C).astype(jnp.float32), probe.astype(jnp.float32),
                     precision=lax.Precision.HIGHEST, preferred_element_type=jnp.float32)
    return stored, sketch.reshape(2 * NBLK, BLOCK, PW)
```

```python
import functools

import jax
import jax.numpy as jnp
from jax import lax
from jax.experimental import pallas as pl
from jax.experimental.pallas import tpu as pltpu
from jax.sharding import PartitionSpec as P

R = 8192
BLOCK = 128
TILE = 16
WINDOW = 256
MIB = 1 << 20


def from_behind(block, axis, distance):
    devices = range(lax.axis_size(axis))
    route = [((i - distance) % len(devices), i) for i in devices]
    return lax.ppermute(block, axis, route)


def floor_tile(value):
    return lax.shift_left(lax.shift_right_arithmetic(value, 4), 4)


def edges_kernel(begin_ref, embed_ref, head_ref, lead_ref, trail_ref, sems):
    copies = []
    for m, buffer in enumerate((embed_ref, head_ref)):
        begin = pl.multiple_of(begin_ref[m], TILE)
        copies.append(
            pltpu.make_async_copy(buffer.at[pl.ds(0, lead_ref.shape[1])], lead_ref.at[m], sems.at[2 * m])
        )
        copies.append(
            pltpu.make_async_copy(
                buffer.at[pl.ds(begin, trail_ref.shape[1])], trail_ref.at[m], sems.at[2 * m + 1]
            )
        )
    for copy in copies:
        copy.start()
    for copy in copies:
        copy.wait()


def pack_kernel(per_rank, per_step, picked_ref, meta_ref, embed_ref, head_ref, left_ref, right_ref,
                out_ref, rows, edge, sems):
    height = embed_ref.shape[0]
    left_rows, right_rows = left_ref.shape[1], right_ref.shape[1]
    step = pl.program_id(0)

    @pl.when(step == 0)
    def _():
        copies = []
        for m, buffer in enumerate((embed_ref, head_ref)):
            copies.append(
                pltpu.make_async_copy(buffer, rows.at[pl.ds(m * height, height)], sems.at[3 * m])
            )
            copies.append(
                pltpu.make_async_copy(
                    left_ref.at[m], edge.at[pl.ds(m * left_rows, left_rows)], sems.at[3 * m + 1]
                )
            )
            copies.append(
                pltpu.make_async_copy(
                    right_ref.at[m],
                    edge.at[pl.ds(2 * left_rows + m * right_rows, right_rows)],
                    sems.at[3 * m + 2],
                )
            )
        for copy in copies:
            copy.start()
        for copy in copies:
            copy.wait()

    row = lax.broadcasted_iota(jnp.int32, (BLOCK, WINDOW), 0)
    ahead = lax.broadcasted_iota(jnp.int32, (BLOCK, WINDOW), 1) - row

    def place(offset, low, high, window):
        chosen = (ahead == offset) & (row >= low) & (row < high)
        selector = jnp.where(chosen, 1.0, 0.0).astype(jnp.bfloat16)
        return jnp.dot(selector, window, preferred_element_type=jnp.float32).astype(jnp.bfloat16)

    for q in range(per_step):
        block = picked_ref[step * per_step + q]
        m = (block >= per_rank).astype(jnp.int32)
        first = (block - m * per_rank) * BLOCK
        before, after, skew = meta_ref[m, 0], meta_ref[m, 1], meta_ref[m, 2]
        start = first - before
        base = jnp.clip(floor_tile(start), 0, height - WINDOW)
        window = rows[pl.ds(pl.multiple_of(m * height + base, TILE), WINDOW), :]
        out_ref[q] = place(start - base, before - first, after - first, window)

        @pl.when((first < before) | (first + BLOCK > after))
        def _():
            is_left = first < before
            begin = jnp.where(is_left, first + skew, first - after)
            limit = jnp.where(is_left, left_rows, right_rows) - WINDOW
            part = jnp.where(is_left, m * left_rows, 2 * left_rows + m * right_rows)
            base = jnp.clip(floor_tile(begin), 0, limit)
            window = edge[pl.ds(pl.multiple_of(part + base, TILE), WINDOW), :]
            low = jnp.where(is_left, 0, after - first)
            high = jnp.where(is_left, before - first, BLOCK)
            out_ref[q] = out_ref[q] + place(begin - base, low, high, window)


def finish_kernel(n_data, per_step, position_ref, incoming_ref, probe_ref, stored_ref, sketch_ref):
    width = incoming_ref.shape[2]
    step = pl.program_id(0)
    for q in range(per_step):
        for d in range(n_data):
            where = position_ref[(step * per_step + q) * n_data + d]
            stored_ref[q, :, d * width : (d + 1) * width] = incoming_ref[where]
        sketch_ref[q] = jnp.dot(
            stored_ref[q], probe_ref[...], preferred_element_type=jnp.float32
        )


def edges(begin, embed_rows, head_rows, quarter):
    width = embed_rows.shape[1]
    kind = embed_rows.dtype
    whole = pl.BlockSpec(memory_space=pltpu.VMEM)
    return pl.pallas_call(
        edges_kernel,
        grid_spec=pltpu.PrefetchScalarGridSpec(
            num_scalar_prefetch=1,
            grid=(),
            in_specs=[pl.BlockSpec(memory_space=pl.ANY)] * 2,
            out_specs=[whole, whole],
            scratch_shapes=[pltpu.SemaphoreType.DMA((4,))],
        ),
        out_shape=[
            jax.ShapeDtypeStruct((2, quarter, width), kind),
            jax.ShapeDtypeStruct((2, quarter + TILE, width), kind),
        ],
        name="edges",
    )(begin, embed_rows, head_rows)


def pack(picked, meta, embed_rows, head_rows, from_left, from_right):
    height, width = embed_rows.shape
    count = picked.shape[0]
    per_step = 16
    kind = embed_rows.dtype
    return pl.pallas_call(
        functools.partial(pack_kernel, R // BLOCK, per_step),
        grid_spec=pltpu.PrefetchScalarGridSpec(
            num_scalar_prefetch=2,
            grid=(count // per_step,),
            in_specs=[pl.BlockSpec(memory_space=pl.ANY)] * 4,
            out_specs=pl.BlockSpec((per_step, BLOCK, width), lambda i, *_: (i, 0, 0)),
            scratch_shapes=[
                pltpu.VMEM((2 * height, width), kind),
                pltpu.VMEM((2 * (from_left.shape[1] + from_right.shape[1]), width), kind),
                pltpu.SemaphoreType.DMA((6,)),
            ],
        ),
        out_shape=jax.ShapeDtypeStruct((count, BLOCK, width), kind),
        compiler_params=pltpu.CompilerParams(dimension_semantics=("arbitrary",)),
        name="pack",
    )(picked, meta, embed_rows, head_rows, from_left, from_right)


def finish(position, incoming, probe, slot_count, n_data):
    width = incoming.shape[2]
    columns, sketch_width = probe.shape
    per_step = 4
    return pl.pallas_call(
        functools.partial(finish_kernel, n_data, per_step),
        grid_spec=pltpu.PrefetchScalarGridSpec(
            num_scalar_prefetch=1,
            grid=(slot_count // per_step,),
            in_specs=[
                pl.BlockSpec(incoming.shape, lambda i, *_: (0, 0, 0)),
                pl.BlockSpec(probe.shape, lambda i, *_: (0, 0)),
            ],
            out_specs=[
                pl.BlockSpec((per_step, BLOCK, columns), lambda i, *_: (i, 0, 0)),
                pl.BlockSpec((per_step, BLOCK, sketch_width), lambda i, *_: (i, 0, 0)),
            ],
        ),
        out_shape=[
            jax.ShapeDtypeStruct((slot_count, BLOCK, columns), incoming.dtype),
            jax.ShapeDtypeStruct((slot_count, BLOCK, sketch_width), jnp.float32),
        ],
        compiler_params=pltpu.CompilerParams(
            dimension_semantics=("arbitrary",), vmem_limit_bytes=48 * MIB
        ),
        name="finish",
    )(position, incoming, probe)


def shards(embed_rows, head_rows, row_offsets, slot_table, probe):
    n_tensor = lax.axis_size("tensor")
    n_data = lax.axis_size("dp")
    my_tensor = lax.axis_index("tensor")
    my_data = lax.axis_index("dp")
    quarter = R // 4
    height = embed_rows.shape[0]

    def tail_begin(rank):
        return jnp.clip((rank + 1) * R - row_offsets[:, rank], 0, height - quarter - 1)

    begin = floor_tile(tail_begin(my_tensor))
    lead_part, trail_part = edges(begin, embed_rows, head_rows, quarter)
    from_left = from_behind(trail_part, "tensor", 1)
    from_right = from_behind(lead_part, "tensor", -1)
    left_begin = tail_begin((my_tensor + n_tensor - 1) % n_tensor)
    skew = left_begin - floor_tile(left_begin)
    meta = jnp.stack(
        [row_offsets[:, my_tensor] - my_tensor * R, row_offsets[:, my_tensor + 1] - my_tensor * R, skew], axis=1
    )

    devices = n_tensor * n_data
    per_rank = R // BLOCK
    total_blocks = per_rank * n_tensor
    slot_count = 2 * total_blocks // devices
    max_from = slot_count // n_tensor
    slot_grid = slot_table.reshape(devices, slot_count)
    source = slot_grid % total_blocks // per_rank
    local_block = slot_grid // total_blocks * per_rank + slot_grid % per_rank
    from_me = source == my_tensor
    slot_range = jnp.arange(slot_count, dtype=jnp.int32)
    lower = slot_range[None, :] < slot_range[:, None]
    rank_order = jnp.sum((from_me[:, None, :] & lower[None]).astype(jnp.int32), axis=2)
    slot_index = jnp.arange(max_from, dtype=jnp.int32)
    select = from_me[:, None, :] & (rank_order[:, None, :] == slot_index[None, :, None])
    picked = jnp.sum(jnp.where(select, local_block[:, None, :], 0), axis=2).reshape(-1)
    writer = my_data * n_tensor + my_tensor
    my_source = source[writer]
    earlier = (my_source[None, :] == my_source[:, None]) & lower
    rank_within = jnp.sum(earlier.astype(jnp.int32), axis=1)
    data_range = jnp.arange(n_data, dtype=jnp.int32)
    position = (
        (data_range[None, :] * n_tensor + my_source[:, None]) * max_from + rank_within[:, None]
    ).reshape(-1)

    outgoing = pack(picked, meta, embed_rows, head_rows, from_left, from_right)
    incoming = lax.all_to_all(outgoing, ("dp", "tensor"), split_axis=0, concat_axis=0, tiled=True)
    stored, sketch = finish(position, incoming, probe, slot_count, n_data)
    return (stored, sketch)


def solution(mesh):
    return jax.shard_map(
        shards,
        mesh=mesh,
        in_specs=(P("tensor", "dp"), P("tensor", "dp"), P(), P(), P()),
        out_specs=(P(("dp", "tensor"), None, None), P(("dp", "tensor"), None, None)),
        check_vma=False,
    )
```

```python
import functools

import jax
import jax.numpy as jnp
from jax import lax
from jax.experimental import pallas as pl
from jax.experimental.pallas import tpu as pltpu
from jax.sharding import PartitionSpec as P

R = 8192
BLOCK = 128
TILE = 16
WINDOW = 256
MIB = 1 << 20


def from_behind(block, axis, distance):
    devices = range(lax.axis_size(axis))
    route = [((i - distance) % len(devices), i) for i in devices]
    return lax.ppermute(block, axis, route)


def floor_tile(value):
    return lax.shift_left(lax.shift_right_arithmetic(value, 4), 4)


def tail_begin(offset, rank, height, quarter):
    return jnp.clip((rank + 1) * R - offset, 0, height - quarter - 1)


def selector(offset):
    row = lax.broadcasted_iota(jnp.int32, (BLOCK, WINDOW), 0)
    column = lax.broadcasted_iota(jnp.int32, (BLOCK, WINDOW), 1)
    return jnp.where(column - row == offset, 1.0, 0.0).astype(jnp.bfloat16)


def place(offset, window):
    moved = jnp.dot(selector(offset), window, preferred_element_type=jnp.float32)
    return moved.astype(window.dtype)


def edges_kernel(offsets_ref, embed_ref, head_ref, lead_ref, trail_ref, sems):
    rank = lax.axis_index("tensor")
    copies = []
    for m, buffer in enumerate((embed_ref, head_ref)):
        begin = floor_tile(
            tail_begin(offsets_ref[m, rank], rank, buffer.shape[0], lead_ref.shape[1])
        )
        begin = pl.multiple_of(begin, TILE)
        copies.append(
            pltpu.make_async_copy(buffer.at[pl.ds(0, lead_ref.shape[1])], lead_ref.at[m], sems.at[2 * m])
        )
        copies.append(
            pltpu.make_async_copy(
                buffer.at[pl.ds(begin, trail_ref.shape[1])], trail_ref.at[m], sems.at[2 * m + 1]
            )
        )
    for copy in copies:
        copy.start()
    for copy in copies:
        copy.wait()


def pack_kernel(per_rank, per_step, picked_ref, meta_ref, embed_ref, head_ref, out_ref, rows, sems):
    height = embed_ref.shape[0]
    step = pl.program_id(0)

    @pl.when(step == 0)
    def _():
        copies = [
            pltpu.make_async_copy(buffer, rows.at[pl.ds(m * height, height)], sems.at[m])
            for m, buffer in enumerate((embed_ref, head_ref))
        ]
        for copy in copies:
            copy.start()
        for copy in copies:
            copy.wait()

    for q in range(per_step):
        block = picked_ref[step * per_step + q]
        m = (block >= per_rank).astype(jnp.int32)
        start = (block - m * per_rank) * BLOCK - meta_ref[m, 0]
        base = jnp.clip(floor_tile(start), 0, height - WINDOW)
        window = rows[pl.ds(pl.multiple_of(m * height + base, TILE), WINDOW), :]
        out_ref[q] = place(start - base, window)


def fix_kernel(per_rank, group, slots_ref, count_ref, picked_ref, meta_ref, packed_ref, left_ref, right_ref,
               out_ref, work, get_sems, put_sems):
    del packed_ref
    count = count_ref[0]

    def get(k):
        return pltpu.make_async_copy(out_ref.at[slots_ref[k]], work.at[k], get_sems.at[k])

    def put(k):
        return pltpu.make_async_copy(work.at[k], out_ref.at[slots_ref[k]], put_sems.at[k])

    def span(g):
        return g * group, jnp.minimum(count, (g + 1) * group)

    def start_get(k, carry):
        get(k).start()
        return carry

    def wait_get(k, carry):
        get(k).wait()
        return carry

    def start_put(k, carry):
        put(k).start()
        return carry

    def wait_put(k, carry):
        put(k).wait()
        return carry

    lax.fori_loop(0, count, start_get, 0)
    row = lax.broadcasted_iota(jnp.int32, (BLOCK, work.shape[2]), 0)

    def one_group(g, carry):
        low_k, high_k = span(g)
        lax.fori_loop(low_k, high_k, wait_get, 0)
        for q in range(group):
            k = g * group + q
            block = picked_ref[slots_ref[k]]
            m = (block >= per_rank).astype(jnp.int32)
            first = (block - m * per_rank) * BLOCK
            before, after, skew = meta_ref[m, 0], meta_ref[m, 1], meta_ref[m, 2]
            is_left = first < before
            left_base = jnp.clip(floor_tile(first + skew), 0, left_ref.shape[1] - WINDOW)
            right_base = jnp.clip(floor_tile(first - after), 0, right_ref.shape[1] - WINDOW)
            window = jnp.where(
                is_left,
                left_ref[m, pl.ds(pl.multiple_of(left_base, TILE), WINDOW), :],
                right_ref[m, pl.ds(pl.multiple_of(right_base, TILE), WINDOW), :],
            )
            offset = jnp.where(is_left, first + skew - left_base, first - after - right_base)
            low = jnp.where(is_left, 0, after - first)
            high = jnp.where(is_left, before - first, BLOCK)
            moved = jnp.dot(selector(offset), window, preferred_element_type=jnp.float32)
            kept = work[k].astype(jnp.float32)
            work[k] = jnp.where((row >= low) & (row < high), moved, kept).astype(work.dtype)
        lax.fori_loop(low_k, high_k, start_put, 0)
        return carry

    lax.fori_loop(0, (count + group - 1) // group, one_group, 0)
    lax.fori_loop(0, count, wait_put, 0)


def finish_kernel(n_data, per_step, position_ref, incoming_ref, probe_ref, stored_ref, sketch_ref, slots, sems):
    width = incoming_ref.shape[2]
    step = pl.program_id(0)
    steps = pl.num_programs(0)
    depth = slots.shape[0]

    def copies(s):
        place_of = lax.rem(s, depth)
        return [
            pltpu.make_async_copy(
                incoming_ref.at[position_ref[(s * per_step + q) * n_data + d]],
                slots.at[place_of, q, :, pl.ds(d * width, width)],
                sems.at[place_of, q * n_data + d],
            )
            for q in range(per_step)
            for d in range(n_data)
        ]

    @pl.when(step == 0)
    def _():
        for s in range(depth - 1):
            for copy in copies(s):
                copy.start()

    @pl.when(step + depth - 1 < steps)
    def _():
        for copy in copies(step + depth - 1):
            copy.start()

    for copy in copies(step):
        copy.wait()
    here = lax.rem(step, depth)
    for q in range(per_step):
        stored_ref[q] = slots[here, q]
        sketch_ref[q] = jnp.dot(slots[here, q], probe_ref[...], preferred_element_type=jnp.float32)


def edges(row_offsets, embed_rows, head_rows, quarter):
    width = embed_rows.shape[1]
    kind = embed_rows.dtype
    whole = pl.BlockSpec(memory_space=pltpu.VMEM)
    return pl.pallas_call(
        edges_kernel,
        grid_spec=pltpu.PrefetchScalarGridSpec(
            num_scalar_prefetch=1,
            grid=(),
            in_specs=[pl.BlockSpec(memory_space=pl.ANY)] * 2,
            out_specs=[whole, whole],
            scratch_shapes=[pltpu.SemaphoreType.DMA((4,))],
        ),
        out_shape=[
            jax.ShapeDtypeStruct((2, quarter, width), kind),
            jax.ShapeDtypeStruct((2, quarter + TILE, width), kind),
        ],
        name="edges",
    )(row_offsets, embed_rows, head_rows)


def pack(picked, meta, embed_rows, head_rows):
    height, width = embed_rows.shape
    count = picked.shape[0]
    per_step = 16
    kind = embed_rows.dtype
    return pl.pallas_call(
        functools.partial(pack_kernel, R // BLOCK, per_step),
        grid_spec=pltpu.PrefetchScalarGridSpec(
            num_scalar_prefetch=2,
            grid=(count // per_step,),
            in_specs=[pl.BlockSpec(memory_space=pl.ANY)] * 2,
            out_specs=pl.BlockSpec((per_step, BLOCK, width), lambda i, *_: (i, 0, 0)),
            scratch_shapes=[
                pltpu.VMEM((2 * height, width), kind),
                pltpu.SemaphoreType.DMA((2,)),
            ],
        ),
        out_shape=jax.ShapeDtypeStruct((count, BLOCK, width), kind),
        compiler_params=pltpu.CompilerParams(
            dimension_semantics=("arbitrary",), vmem_limit_bytes=24 * MIB
        ),
        cost_estimate=pl.CostEstimate(
            flops=2 * count * BLOCK * WINDOW * width, bytes_accessed=24 * MIB, transcendentals=0
        ),
        name="pack",
    )(picked, meta, embed_rows, head_rows)


def fix(slots, count, picked, meta, packed, from_left, from_right):
    most, group = slots.shape[0], 8
    return pl.pallas_call(
        functools.partial(fix_kernel, R // BLOCK, group),
        grid_spec=pltpu.PrefetchScalarGridSpec(
            num_scalar_prefetch=4,
            grid=(),
            in_specs=[
                pl.BlockSpec(memory_space=pltpu.HBM),
                pl.BlockSpec(memory_space=pltpu.VMEM),
                pl.BlockSpec(memory_space=pltpu.VMEM),
            ],
            out_specs=pl.BlockSpec(memory_space=pltpu.HBM),
            scratch_shapes=[
                pltpu.VMEM((most,) + packed.shape[1:], packed.dtype),
                pltpu.SemaphoreType.DMA((most,)),
                pltpu.SemaphoreType.DMA((most,)),
            ],
        ),
        out_shape=jax.ShapeDtypeStruct(packed.shape, packed.dtype),
        input_output_aliases={4: 0},
        compiler_params=pltpu.CompilerParams(vmem_limit_bytes=24 * MIB),
        name="fix",
    )(slots, count, picked, meta, packed, from_left, from_right)


def finish(position, incoming, probe, slot_count, n_data):
    columns, sketch_width = probe.shape
    per_step, depth = 2, 4
    return pl.pallas_call(
        functools.partial(finish_kernel, n_data, per_step),
        grid_spec=pltpu.PrefetchScalarGridSpec(
            num_scalar_prefetch=1,
            grid=(slot_count // per_step,),
            in_specs=[
                pl.BlockSpec(memory_space=pl.ANY),
                pl.BlockSpec(probe.shape, lambda i, *_: (0, 0)),
            ],
            out_specs=[
                pl.BlockSpec((per_step, BLOCK, columns), lambda i, *_: (i, 0, 0)),
                pl.BlockSpec((per_step, BLOCK, sketch_width), lambda i, *_: (i, 0, 0)),
            ],
            scratch_shapes=[
                pltpu.VMEM((depth, per_step, BLOCK, columns), incoming.dtype),
                pltpu.SemaphoreType.DMA((depth, per_step * n_data)),
            ],
        ),
        out_shape=[
            jax.ShapeDtypeStruct((slot_count, BLOCK, columns), incoming.dtype),
            jax.ShapeDtypeStruct((slot_count, BLOCK, sketch_width), jnp.float32),
        ],
        compiler_params=pltpu.CompilerParams(
            dimension_semantics=("arbitrary",), vmem_limit_bytes=32 * MIB
        ),
        name="finish",
    )(position, incoming, probe)


def shards(embed_rows, head_rows, row_offsets, slot_table, probe):
    n_tensor = lax.axis_size("tensor")
    n_data = lax.axis_size("dp")
    my_tensor = lax.axis_index("tensor")
    my_data = lax.axis_index("dp")
    quarter = R // 4
    height = embed_rows.shape[0]

    lead_part, trail_part = edges(row_offsets, embed_rows, head_rows, quarter)
    from_left = from_behind(trail_part, "tensor", 1)
    from_right = from_behind(lead_part, "tensor", -1)
    left = (my_tensor + n_tensor - 1) % n_tensor
    left_begin = tail_begin(row_offsets[:, left], left, height, quarter)
    skew = left_begin - floor_tile(left_begin)
    meta = jnp.stack(
        [row_offsets[:, my_tensor] - my_tensor * R, row_offsets[:, my_tensor + 1] - my_tensor * R, skew], axis=1
    )

    devices = n_tensor * n_data
    per_rank = R // BLOCK
    total_blocks = per_rank * n_tensor
    slot_count = 2 * total_blocks // devices
    max_from = slot_count // n_tensor
    slot_grid = slot_table.reshape(devices, slot_count)
    source = slot_grid % total_blocks // per_rank
    local_block = slot_grid // total_blocks * per_rank + slot_grid % per_rank
    from_me = source == my_tensor
    slot_range = jnp.arange(slot_count, dtype=jnp.int32)
    lower = slot_range[None, :] < slot_range[:, None]
    rank_order = jnp.sum((from_me[:, None, :] & lower[None]).astype(jnp.int32), axis=2)
    slot_index = jnp.arange(max_from, dtype=jnp.int32)
    select = from_me[:, None, :] & (rank_order[:, None, :] == slot_index[None, :, None])
    picked = jnp.sum(jnp.where(select, local_block[:, None, :], 0), axis=2).reshape(-1)
    writer = my_data * n_tensor + my_tensor
    my_source = source[writer]
    earlier = (my_source[None, :] == my_source[:, None]) & lower
    rank_within = jnp.sum(earlier.astype(jnp.int32), axis=1)
    data_range = jnp.arange(n_data, dtype=jnp.int32)
    position = (
        (data_range[None, :] * n_tensor + my_source[:, None]) * max_from + rank_within[:, None]
    ).reshape(-1)

    matrix = picked // per_rank
    first = picked % per_rank * BLOCK
    before = jnp.where(matrix == 0, meta[0, 0], meta[1, 0])
    after = jnp.where(matrix == 0, meta[0, 1], meta[1, 1])
    on_edge = (first < before) | (first + BLOCK > after)
    everything = jnp.arange(picked.shape[0], dtype=jnp.int32)
    turn = jnp.sum((on_edge[None, :] & (everything[None, :] < everything[:, None])).astype(jnp.int32), axis=1)
    most = jnp.arange(4 * quarter // BLOCK, dtype=jnp.int32)
    slots = jnp.sum(
        jnp.where(on_edge[None, :] & (turn[None, :] == most[:, None]), everything[None, :], 0), axis=1
    )
    count = jnp.sum(on_edge.astype(jnp.int32)).reshape(1)

    packed = pack(picked, meta, embed_rows, head_rows)
    outgoing = fix(slots, count, picked, meta, packed, from_left, from_right)
    incoming = lax.all_to_all(outgoing, ("dp", "tensor"), split_axis=0, concat_axis=0, tiled=True)
    stored, sketch = finish(position, incoming, probe, slot_count, n_data)
    return (stored, sketch)


def solution(mesh):
    return jax.shard_map(
        shards,
        mesh=mesh,
        in_specs=(P("tensor", "dp"), P("tensor", "dp"), P(), P(), P()),
        out_specs=(P(("dp", "tensor"), None, None), P(("dp", "tensor"), None, None)),
        check_vma=False,
    )
```

```python
import functools

import jax
import jax.numpy as jnp
from jax import lax
from jax.experimental import pallas as pl
from jax.experimental.pallas import tpu as pltpu
from jax.sharding import PartitionSpec as P

R = 8192
BLOCK = 128
TILE = 16
WINDOW = 256
MIB = 1 << 20


def from_behind(block, axis, distance):
    devices = range(lax.axis_size(axis))
    route = [((i - distance) % len(devices), i) for i in devices]
    return lax.ppermute(block, axis, route)


def floor_tile(value):
    return lax.shift_left(lax.shift_right_arithmetic(value, 4), 4)


def tail_begin(offset, rank, height, quarter):
    return jnp.clip((rank + 1) * R - offset, 0, height - quarter - 1)


def selector(offset):
    row = lax.broadcasted_iota(jnp.int32, (BLOCK, WINDOW), 0)
    column = lax.broadcasted_iota(jnp.int32, (BLOCK, WINDOW), 1)
    return jnp.where(column - row == offset, 1.0, 0.0).astype(jnp.bfloat16)


def place(offset, window):
    moved = jnp.dot(selector(offset), window, preferred_element_type=jnp.float32)
    return moved.astype(window.dtype)


def edges_kernel(offsets_ref, embed_ref, head_ref, lead_ref, trail_ref, sems):
    rank = lax.axis_index("tensor")
    copies = []
    for m, buffer in enumerate((embed_ref, head_ref)):
        begin = floor_tile(
            tail_begin(offsets_ref[m, rank], rank, buffer.shape[0], lead_ref.shape[1])
        )
        begin = pl.multiple_of(begin, TILE)
        copies.append(
            pltpu.make_async_copy(buffer.at[pl.ds(0, lead_ref.shape[1])], lead_ref.at[m], sems.at[2 * m])
        )
        copies.append(
            pltpu.make_async_copy(
                buffer.at[pl.ds(begin, trail_ref.shape[1])], trail_ref.at[m], sems.at[2 * m + 1]
            )
        )
    for copy in copies:
        copy.start()
    for copy in copies:
        copy.wait()


def pack_kernel(per_rank, per_step, picked_ref, meta_ref, embed_ref, head_ref, out_ref, rows, sems):
    height = embed_ref.shape[0]
    step = pl.program_id(0)

    @pl.when(step == 0)
    def _():
        copies = [
            pltpu.make_async_copy(buffer, rows.at[pl.ds(m * height, height)], sems.at[m])
            for m, buffer in enumerate((embed_ref, head_ref))
        ]
        for copy in copies:
            copy.start()
        for copy in copies:
            copy.wait()

    for q in range(per_step):
        block = picked_ref[step * per_step + q]
        m = (block >= per_rank).astype(jnp.int32)
        start = (block - m * per_rank) * BLOCK - meta_ref[m, 0]
        base = jnp.clip(floor_tile(start), 0, height - WINDOW)
        window = rows[pl.ds(pl.multiple_of(m * height + base, TILE), WINDOW), :]
        out_ref[q] = place(start - base, window)


def fix_kernel(per_rank, group, slots_ref, count_ref, picked_ref, meta_ref, packed_ref, left_ref, right_ref,
               out_ref, work, sems):
    count = count_ref[0]
    total = out_ref.shape[0]

    def keep(k):
        return pltpu.make_async_copy(packed_ref.at[slots_ref[k]], out_ref.at[slots_ref[k]], sems.at[k])

    def put(k):
        return pltpu.make_async_copy(work.at[k], out_ref.at[slots_ref[k]], sems.at[k])

    def start_keep(k, carry):
        keep(k).start()
        return carry

    def wait_keep(k, carry):
        keep(k).wait()
        return carry

    def start_put(k, carry):
        put(k).start()
        return carry

    def wait_put(k, carry):
        put(k).wait()
        return carry

    lax.fori_loop(count, total, start_keep, 0)
    row = lax.broadcasted_iota(jnp.int32, (BLOCK, work.shape[2]), 0)

    def one_group(g, carry):
        for q in range(group):
            k = g * group + q
            block = picked_ref[slots_ref[k]]
            m = (block >= per_rank).astype(jnp.int32)
            first = (block - m * per_rank) * BLOCK
            before, after, skew = meta_ref[m, 0], meta_ref[m, 1], meta_ref[m, 2]
            is_left = first < before
            left_base = jnp.clip(floor_tile(first + skew), 0, left_ref.shape[1] - WINDOW)
            right_base = jnp.clip(floor_tile(first - after), 0, right_ref.shape[1] - WINDOW)
            window = jnp.where(
                is_left,
                left_ref[m, pl.ds(pl.multiple_of(left_base, TILE), WINDOW), :],
                right_ref[m, pl.ds(pl.multiple_of(right_base, TILE), WINDOW), :],
            )
            offset = jnp.where(is_left, first + skew - left_base, first - after - right_base)
            low = jnp.where(is_left, 0, after - first)
            high = jnp.where(is_left, before - first, BLOCK)
            moved = jnp.dot(selector(offset), window, preferred_element_type=jnp.float32)
            kept = packed_ref[slots_ref[k]].astype(jnp.float32)
            work[k] = jnp.where((row >= low) & (row < high), moved, kept).astype(work.dtype)
        lax.fori_loop(g * group, jnp.minimum(count, (g + 1) * group), start_put, 0)
        return carry

    lax.fori_loop(0, (count + group - 1) // group, one_group, 0)
    lax.fori_loop(0, count, wait_put, 0)
    lax.fori_loop(count, total, wait_keep, 0)


def finish_kernel(n_data, per_step, position_ref, incoming_ref, probe_ref, stored_ref, sketch_ref):
    width = incoming_ref.shape[2]
    step = pl.program_id(0)
    for q in range(per_step):
        for d in range(n_data):
            where = position_ref[(step * per_step + q) * n_data + d]
            stored_ref[q, :, d * width : (d + 1) * width] = incoming_ref[where]
    rows = stored_ref[...].reshape(per_step * BLOCK, n_data * width)
    product = jnp.dot(rows, probe_ref[...], preferred_element_type=jnp.float32)
    sketch_ref[...] = product.reshape(sketch_ref.shape)


def edges(row_offsets, embed_rows, head_rows, quarter):
    width = embed_rows.shape[1]
    kind = embed_rows.dtype
    whole = pl.BlockSpec(memory_space=pltpu.VMEM)
    return pl.pallas_call(
        edges_kernel,
        grid_spec=pltpu.PrefetchScalarGridSpec(
            num_scalar_prefetch=1,
            grid=(),
            in_specs=[pl.BlockSpec(memory_space=pl.ANY)] * 2,
            out_specs=[whole, whole],
            scratch_shapes=[pltpu.SemaphoreType.DMA((4,))],
        ),
        out_shape=[
            jax.ShapeDtypeStruct((2, quarter, width), kind),
            jax.ShapeDtypeStruct((2, quarter + TILE, width), kind),
        ],
        name="edges",
    )(row_offsets, embed_rows, head_rows)


def pack(picked, meta, embed_rows, head_rows):
    height, width = embed_rows.shape
    count = picked.shape[0]
    per_step = 16
    kind = embed_rows.dtype
    return pl.pallas_call(
        functools.partial(pack_kernel, R // BLOCK, per_step),
        grid_spec=pltpu.PrefetchScalarGridSpec(
            num_scalar_prefetch=2,
            grid=(count // per_step,),
            in_specs=[pl.BlockSpec(memory_space=pl.ANY)] * 2,
            out_specs=pl.BlockSpec((per_step, BLOCK, width), lambda i, *_: (i, 0, 0)),
            scratch_shapes=[
                pltpu.VMEM((2 * height, width), kind),
                pltpu.SemaphoreType.DMA((2,)),
            ],
        ),
        out_shape=jax.ShapeDtypeStruct((count, BLOCK, width), kind),
        compiler_params=pltpu.CompilerParams(
            dimension_semantics=("arbitrary",), vmem_limit_bytes=24 * MIB
        ),
        cost_estimate=pl.CostEstimate(
            flops=2 * count * BLOCK * WINDOW * width, bytes_accessed=24 * MIB, transcendentals=0
        ),
        name="pack",
    )(picked, meta, embed_rows, head_rows)


def fix(slots, count, picked, meta, packed, from_left, from_right):
    most, group = 4 * (R // 4) // BLOCK, 8
    return pl.pallas_call(
        functools.partial(fix_kernel, R // BLOCK, group),
        grid_spec=pltpu.PrefetchScalarGridSpec(
            num_scalar_prefetch=4,
            grid=(),
            in_specs=[
                pl.BlockSpec(memory_space=pltpu.VMEM),
                pl.BlockSpec(memory_space=pltpu.VMEM),
                pl.BlockSpec(memory_space=pltpu.VMEM),
            ],
            out_specs=pl.BlockSpec(memory_space=pl.ANY),
            scratch_shapes=[
                pltpu.VMEM((most,) + packed.shape[1:], packed.dtype),
                pltpu.SemaphoreType.DMA((packed.shape[0],)),
            ],
        ),
        out_shape=jax.ShapeDtypeStruct(packed.shape, packed.dtype),
        compiler_params=pltpu.CompilerParams(vmem_limit_bytes=57 * MIB),
        name="fix",
    )(slots, count, picked, meta, packed, from_left, from_right)


def finish(position, incoming, probe, slot_count, n_data):
    columns, sketch_width = probe.shape
    per_step = 4
    return pl.pallas_call(
        functools.partial(finish_kernel, n_data, per_step),
        grid_spec=pltpu.PrefetchScalarGridSpec(
            num_scalar_prefetch=1,
            grid=(slot_count // per_step,),
            in_specs=[
                pl.BlockSpec(incoming.shape, lambda i, *_: (0, 0, 0)),
                pl.BlockSpec(probe.shape, lambda i, *_: (0, 0)),
            ],
            out_specs=[
                pl.BlockSpec((per_step, BLOCK, columns), lambda i, *_: (i, 0, 0)),
                pl.BlockSpec((per_step, BLOCK, sketch_width), lambda i, *_: (i, 0, 0)),
            ],
        ),
        out_shape=[
            jax.ShapeDtypeStruct((slot_count, BLOCK, columns), incoming.dtype),
            jax.ShapeDtypeStruct((slot_count, BLOCK, sketch_width), jnp.float32),
        ],
        compiler_params=pltpu.CompilerParams(
            dimension_semantics=("arbitrary",), vmem_limit_bytes=48 * MIB
        ),
        name="finish",
    )(position, incoming, probe)


def shards(embed_rows, head_rows, row_offsets, slot_table, probe):
    n_tensor = lax.axis_size("tensor")
    n_data = lax.axis_size("dp")
    my_tensor = lax.axis_index("tensor")
    my_data = lax.axis_index("dp")
    quarter = R // 4
    height = embed_rows.shape[0]

    lead_part, trail_part = edges(row_offsets, embed_rows, head_rows, quarter)
    from_left = from_behind(trail_part, "tensor", 1)
    from_right = from_behind(lead_part, "tensor", -1)
    left = (my_tensor + n_tensor - 1) % n_tensor
    left_begin = tail_begin(row_offsets[:, left], left, height, quarter)
    skew = left_begin - floor_tile(left_begin)
    meta = jnp.stack(
        [row_offsets[:, my_tensor] - my_tensor * R, row_offsets[:, my_tensor + 1] - my_tensor * R, skew], axis=1
    )

    devices = n_tensor * n_data
    per_rank = R // BLOCK
    total_blocks = per_rank * n_tensor
    slot_count = 2 * total_blocks // devices
    max_from = slot_count // n_tensor
    slot_grid = slot_table.reshape(devices, slot_count)
    source = slot_grid % total_blocks // per_rank
    local_block = slot_grid // total_blocks * per_rank + slot_grid % per_rank
    from_me = source == my_tensor
    slot_range = jnp.arange(slot_count, dtype=jnp.int32)
    lower = slot_range[None, :] < slot_range[:, None]
    rank_order = jnp.sum((from_me[:, None, :] & lower[None]).astype(jnp.int32), axis=2)
    slot_index = jnp.arange(max_from, dtype=jnp.int32)
    select = from_me[:, None, :] & (rank_order[:, None, :] == slot_index[None, :, None])
    picked = jnp.sum(jnp.where(select, local_block[:, None, :], 0), axis=2).reshape(-1)
    writer = my_data * n_tensor + my_tensor
    my_source = source[writer]
    earlier = (my_source[None, :] == my_source[:, None]) & lower
    rank_within = jnp.sum(earlier.astype(jnp.int32), axis=1)
    data_range = jnp.arange(n_data, dtype=jnp.int32)
    position = (
        (data_range[None, :] * n_tensor + my_source[:, None]) * max_from + rank_within[:, None]
    ).reshape(-1)

    matrix = picked // per_rank
    first = picked % per_rank * BLOCK
    before = jnp.where(matrix == 0, meta[0, 0], meta[1, 0])
    after = jnp.where(matrix == 0, meta[0, 1], meta[1, 1])
    on_edge = (first < before) | (first + BLOCK > after)
    everything = jnp.arange(picked.shape[0], dtype=jnp.int32)
    ahead = jnp.sum((on_edge[None, :] & (everything[None, :] < everything[:, None])).astype(jnp.int32), axis=1)
    count = jnp.sum(on_edge.astype(jnp.int32)).reshape(1)
    turn = jnp.where(on_edge, ahead, count + everything - ahead)
    slots = jnp.sum(jnp.where(turn[None, :] == everything[:, None], everything[None, :], 0), axis=1)

    packed = pack(picked, meta, embed_rows, head_rows)
    outgoing = fix(slots, count, picked, meta, packed, from_left, from_right)
    incoming = lax.all_to_all(outgoing, ("dp", "tensor"), split_axis=0, concat_axis=0, tiled=True)
    stored, sketch = finish(position, incoming, probe, slot_count, n_data)
    return (stored, sketch)


def solution(mesh):
    return jax.shard_map(
        shards,
        mesh=mesh,
        in_specs=(P("tensor", "dp"), P("tensor", "dp"), P(), P(), P()),
        out_specs=(P(("dp", "tensor"), None, None), P(("dp", "tensor"), None, None)),
        check_vma=False,
    )
```
